16 devices in a mesh: fsdp: 16 (over z, y, x, core).
Axes of the slice: x: 2, y: 2, z: 2, core: 2. Of those that a mesh axis runs over, the one named last changes fastest.
Arguments:
- w_query: float32 [2, 960, 960], P(None, 'fsdp')
- w_key: float32 [2, 960, 320], P(None, 'fsdp')
- w_value: float32 [2, 960, 320], P(None, 'fsdp')
- w_out: float32 [2, 960, 960], P(None, 'fsdp')
- w_gate: float32 [2, 960, 2560], P(None, 'fsdp')
- w_up: float32 [2, 960, 2560], P(None, 'fsdp')
- w_down: float32 [2, 2560, 960], P(None, 'fsdp')
- gain_attn: float32 [2, 960], P(None, 'fsdp')
- gain_mlp: float32 [2, 960], P(None, 'fsdp')
- rope_cos: float32 [256, 32], replicated
- rope_sin: float32 [256, 32], replicated
- x_in: bfloat16 [256, 256, 960], P('fsdp')
- y_cot: bfloat16 [256, 256, 960], P('fsdp')
Outputs:
- output 1: bfloat16 [256, 256, 960], P('fsdp')
- output 2: bfloat16 [256, 256, 960], P('fsdp')
- output 3: float32 [2, 960, 960], P(None, 'fsdp')
- output 4: float32 [2, 960, 320], P(None, 'fsdp')
- output 5: float32 [2, 960, 320], P(None, 'fsdp')
- output 6: float32 [2, 960, 960], P(None, 'fsdp')
- output 7: float32 [2, 960, 2560], P(None, 'fsdp')
- output 8: float32 [2, 960, 2560], P(None, 'fsdp')
- output 9: float32 [2, 2560, 960], P(None, 'fsdp')
- output 10: float32 [2, 960], P(None, 'fsdp')
- output 11: float32 [2, 960], P(None, 'fsdp')
All inputs are finite; a program needn't handle non-finite values.
Results may differ from the reference program's by a relative error of at most 0.02.
Values are sent between devices in bfloat16 or wider.
A program may use at most 1 GiB of HBM per device.

```python
import jax
import jax.numpy as jnp
from jax import lax

MODEL_DIM = 960
FFN_DIM = 2560
HEADS = 15
KV_HEADS = 5
HEAD_DIM = 64
SEQ_LEN = 256
TOTAL_BATCH = 256
LAYERS = 2
NORM_EPS = 1e-5
GROUP_SIZE = HEADS // KV_HEADS
HALF_DIM = HEAD_DIM // 2
Q_WIDTH = HEADS * HEAD_DIM
KV_WIDTH = KV_HEADS * HEAD_DIM


def setup_inputs(seed: int = 0) -> dict:
    key_list = jax.random.split(jax.random.key(seed), 13)

    def draw_weight(rng_key, shape, fan_in):
        return jax.random.normal(rng_key, shape, jnp.float32) * fan_in ** -0.5

    offset = jax.random.randint(key_list[9], (), 0, 4096).astype(jnp.float32)
    jitter = jnp.exp(0.1 * jax.random.normal(key_list[10], (HALF_DIM,), jnp.float32))
    inv_freq = 10000.0 ** (-jnp.arange(HALF_DIM, dtype=jnp.float32) / HALF_DIM) * jitter
    angles = (jnp.arange(SEQ_LEN, dtype=jnp.float32) + offset)[:, None] * inv_freq[None, :]
    tok_shape = (TOTAL_BATCH, SEQ_LEN, MODEL_DIM)
    return {
        "w_query": draw_weight(key_list[0], (LAYERS, MODEL_DIM, Q_WIDTH), MODEL_DIM),
        "w_key": draw_weight(key_list[1], (LAYERS, MODEL_DIM, KV_WIDTH), MODEL_DIM),
        "w_value": draw_weight(key_list[2], (LAYERS, MODEL_DIM, KV_WIDTH), MODEL_DIM),
        "w_out": draw_weight(key_list[3], (LAYERS, Q_WIDTH, MODEL_DIM), Q_WIDTH),
        "w_gate": draw_weight(key_list[4], (LAYERS, MODEL_DIM, FFN_DIM), MODEL_DIM),
        "w_up": draw_weight(key_list[5], (LAYERS, MODEL_DIM, FFN_DIM), MODEL_DIM),
        "w_down": draw_weight(key_list[6], (LAYERS, FFN_DIM, MODEL_DIM), FFN_DIM),
        "gain_attn": 1.0 + 0.2 * jax.random.normal(key_list[7], (LAYERS, MODEL_DIM), jnp.float32),
        "gain_mlp": 1.0 + 0.2 * jax.random.normal(key_list[8], (LAYERS, MODEL_DIM), jnp.float32),
        "rope_cos": jnp.cos(angles),
        "rope_sin": jnp.sin(angles),
        "x_in": jax.random.normal(key_list[11], tok_shape, jnp.float32).astype(jnp.bfloat16),
        "y_cot": jax.random.normal(key_list[12], tok_shape, jnp.float32).astype(jnp.bfloat16),
    }


def rms_norm(values, gain):
    vals32 = values.astype(jnp.float32)
    inv_rms = lax.rsqrt(jnp.mean(vals32 * vals32, axis=-1, keepdims=True) + NORM_EPS)
    return (vals32 * inv_rms * gain.astype(jnp.float32)).astype(jnp.bfloat16)


def apply_rope(heads32, rope_cos, rope_sin):
    first_half = heads32[..., :HALF_DIM]
    second_half = heads32[..., HALF_DIM:]
    cos_b = rope_cos[:, None, :]
    sin_b = rope_sin[:, None, :]
    return jnp.concatenate([first_half * cos_b - second_half * sin_b, second_half * cos_b + first_half * sin_b], axis=-1)


def layer_forward(weights, rope_cos, rope_sin, hidden):
    w_query, w_key, w_value, w_out, w_gate, w_up, w_down, gain_attn, gain_mlp = weights
    normed = rms_norm(hidden, gain_attn)
    q_proj = jnp.dot(normed, w_query, preferred_element_type=jnp.float32).reshape(SEQ_LEN, HEADS, HEAD_DIM)
    q_heads = apply_rope(q_proj, rope_cos, rope_sin).astype(jnp.bfloat16).reshape(SEQ_LEN, KV_HEADS, GROUP_SIZE, HEAD_DIM)
    k_proj = jnp.dot(normed, w_key, preferred_element_type=jnp.float32).reshape(SEQ_LEN, KV_HEADS, HEAD_DIM)
    k_heads = apply_rope(k_proj, rope_cos, rope_sin).astype(jnp.bfloat16)
    v_heads = jnp.dot(normed, w_value, preferred_element_type=jnp.float32).astype(jnp.bfloat16).reshape(SEQ_LEN, KV_HEADS, HEAD_DIM)
    scores = jnp.einsum("qkgd,skd->kgqs", q_heads.astype(jnp.float32), k_heads.astype(jnp.float32)) * HEAD_DIM ** -0.5
    positions = jnp.arange(SEQ_LEN)
    scores = jnp.where(positions[:, None] >= positions[None, :], scores, -1e30)
    attn_probs = jax.nn.softmax(scores, axis=-1).astype(jnp.bfloat16)
    attn_heads = jnp.einsum("kgqs,skd->qkgd", attn_probs.astype(jnp.float32), v_heads.astype(jnp.float32))
    attn_heads = attn_heads.astype(jnp.bfloat16).reshape(SEQ_LEN, Q_WIDTH)
    mid_hidden = (hidden.astype(jnp.float32) + jnp.dot(attn_heads, w_out, preferred_element_type=jnp.float32)).astype(jnp.bfloat16)
    normed_mlp = rms_norm(mid_hidden, gain_mlp)
    gate_pre = jnp.dot(normed_mlp, w_gate, preferred_element_type=jnp.float32)
    up_proj = jnp.dot(normed_mlp, w_up, preferred_element_type=jnp.float32)
    mlp_act = (jax.nn.silu(gate_pre) * up_proj).astype(jnp.bfloat16)
    return (mid_hidden.astype(jnp.float32) + jnp.dot(mlp_act, w_down, preferred_element_type=jnp.float32)).astype(jnp.bfloat16)


def reference(w_query, w_key, w_value, w_out, w_gate, w_up, w_down, gain_attn, gain_mlp, rope_cos, rope_sin, x_in, y_cot):
    masters = (w_query, w_key, w_value, w_out, w_gate, w_up, w_down, gain_attn, gain_mlp)
    params_bf = tuple(master.astype(jnp.bfloat16) for master in masters)

    def stack_forward(params, seq_x):
        def layer_body(hidden, layer_params):
            return layer_forward(layer_params, rope_cos, rope_sin, hidden), None
        return lax.scan(layer_body, seq_x, params)[0]

    def per_sequence(grad_sums, seq_pair):
        seq_x, seq_cot = seq_pair
        seq_y, pullback = jax.vjp(stack_forward, params_bf, seq_x)
        grad_params, grad_x = pullback(seq_cot)
        new_sums = tuple(old_sum + grad_part.astype(jnp.float32) for old_sum, grad_part in zip(grad_sums, grad_params))
        return new_sums, (seq_y, grad_x)

    grad_init = tuple(jnp.zeros(master.shape, jnp.float32) for master in masters)
    grads, outputs = lax.scan(per_sequence, grad_init, (x_in, y_cot))
    return (outputs[0], outputs[1], grads[0], grads[1], grads[2], grads[3], grads[4], grads[5], grads[6], grads[7], grads[8])
```

```python
import functools

import jax
import jax.numpy as jnp
from jax import lax
from jax.experimental import pallas as pl
from jax.experimental.pallas import tpu as pltpu
from jax.sharding import PartitionSpec as P


NORM_EPS = 1e-5
MASK_VALUE = -1e30
F32 = jnp.float32
BF16 = jnp.bfloat16

DEV = 16
D = 960
ROWS = D // DEV
PAD_ROWS = 64
FF = 2560
SHARD_FF = FF // DEV
KV = 320
HD = 64
KVH = 5
GROUP = 3
SEQ = 256
QKV = D + 2 * KV
AW = QKV + D
GAW = 2688
MW = 3 * FF
VMEM_LIMIT = 62 * 1024 * 1024
EXP_SCALE = HD ** -0.5 * 1.4426950408889634


def mm(a, b, ca=1, cb=0):
    return lax.dot_general(a, b, (((ca,), (cb,)), ((), ())), preferred_element_type=F32)


def params(**kw):
    return pltpu.CompilerParams(vmem_limit_bytes=VMEM_LIMIT, dimension_semantics=("arbitrary",), **kw)


def cost(flops, nbytes):
    return pl.CostEstimate(flops=int(flops), bytes_accessed=int(nbytes), transcendentals=0)


def const_spec(shape):
    zeros = (0,) * len(shape)
    return pl.BlockSpec(shape, lambda i: zeros, pipeline_mode=pl.Buffered(1))


ANY = pl.BlockSpec(memory_space=pl.ANY)


def inv_rms_of(vals32):
    return lax.rsqrt(jnp.mean(vals32 * vals32, axis=-1, keepdims=True) + NORM_EPS)


def unpack_shards(raw, buf, sems, place):
    def fetch(d):
        return pltpu.make_async_copy(raw.at[d], buf.at[d % 2], sems.at[d % 2])

    fetch(0).start()
    for d in range(DEV):
        if d + 1 < DEV:
            fetch(d + 1).start()
        fetch(d).wait()
        place(d, buf.at[d % 2])


def probs_t(k_t, q_t):
    scores = mm(k_t.T, q_t) * EXP_SCALE
    key = lax.broadcasted_iota(jnp.int32, scores.shape, 0)
    qry = lax.broadcasted_iota(jnp.int32, scores.shape, 1) & (SEQ - 1)
    scores = jnp.where(key <= qry, scores, MASK_VALUE)
    exps = jnp.exp2(scores - jnp.max(scores, axis=0, keepdims=True))
    return (exps * (1.0 / jnp.sum(exps, axis=0, keepdims=True))).astype(BF16)


def group_cols(ref, kv_head, seq):
    base = kv_head * GROUP * HD
    return jnp.concatenate([ref[base + g * HD: base + (g + 1) * HD, seq * SEQ:(seq + 1) * SEQ] for g in range(GROUP)], axis=1)


def attn_fwd_kernel(seqs, raw, x_ref, gain_ref, cos_ref, sin_ref, h_ref, qkv_ref, o_ref, wqkv_out, wo_out,
                    buf, wqkv_t, wo, sems, out_sems):
    step = pl.program_id(0)
    copies = (pltpu.make_async_copy(wqkv_t, wqkv_out, out_sems.at[0]), pltpu.make_async_copy(wo, wo_out, out_sems.at[1]))

    @pl.when(step == 0)
    def _():
        def place(d, shard):
            wo[d * ROWS:(d + 1) * ROWS, :] = shard[:ROWS, QKV:]
            rows = shard[:, :QKV].T
            wqkv_t[:, d * ROWS:(d + 1) * ROWS] = rows[:, :ROWS]

        unpack_shards(raw, buf, sems, place)
        for copy in copies:
            copy.start()

    x32 = x_ref[...].astype(F32)
    normed = (x32 * inv_rms_of(x32) * gain_ref[...]).astype(BF16)
    cos, sin = cos_ref[...], sin_ref[...]
    half = HD // 2
    for lo in range(0, QKV, KV):
        part = mm(wqkv_t[lo:lo + KV, :], normed, 1, 1)
        if lo < D + KV:
            for head in range(KV // HD):
                a = part[head * HD:head * HD + half]
                b = part[head * HD + half:(head + 1) * HD]
                qkv_ref[lo + head * HD:lo + head * HD + half, :] = (a * cos - b * sin).astype(BF16)
                qkv_ref[lo + head * HD + half:lo + (head + 1) * HD, :] = (b * cos + a * sin).astype(BF16)
        else:
            qkv_ref[lo:lo + KV, :] = part.astype(BF16)
    for seq in range(seqs):
        cols = slice(seq * SEQ, (seq + 1) * SEQ)
        for kvh in range(KVH):
            k_t = qkv_ref[D + kvh * HD:D + (kvh + 1) * HD, cols]
            v_t = qkv_ref[D + KV + kvh * HD:D + KV + (kvh + 1) * HD, cols]
            p_t = probs_t(k_t, group_cols(qkv_ref, kvh, seq))
            o_t = mm(v_t, p_t).astype(BF16)
            for g in range(GROUP):
                row = (kvh * GROUP + g) * HD
                o_ref[row:row + HD, cols] = o_t[:, g * SEQ:(g + 1) * SEQ]
    h_ref[...] = (x32 + mm(o_ref[...].T, wo[...])).astype(BF16)

    @pl.when(step == pl.num_programs(0) - 1)
    def _():
        for copy in copies:
            copy.wait()


def attn_fwd(raw, x, gain, cos_t, sin_t, seqs=2):
    tokens = x.shape[0]
    tm = seqs * SEQ
    row = pl.BlockSpec((tm, D), lambda i: (i, 0))
    col = lambda n: pl.BlockSpec((n, tm), lambda i: (0, i))
    return pl.pallas_call(
        functools.partial(attn_fwd_kernel, seqs),
        grid=(tokens // tm,),
        in_specs=[ANY, row, const_spec((1, D)), const_spec((HD // 2, tm)), const_spec((HD // 2, tm))],
        out_specs=[row, col(QKV), col(D), ANY, ANY],
        out_shape=[jax.ShapeDtypeStruct((tokens, D), BF16), jax.ShapeDtypeStruct((QKV, tokens), BF16),
                   jax.ShapeDtypeStruct((D, tokens), BF16), jax.ShapeDtypeStruct((QKV, D), BF16), jax.ShapeDtypeStruct((D, D), BF16)],
        scratch_shapes=[pltpu.VMEM((2, PAD_ROWS, AW), BF16), pltpu.VMEM((QKV, D), BF16), pltpu.VMEM((D, D), BF16),
                        pltpu.SemaphoreType.DMA((2,)), pltpu.SemaphoreType.DMA((2,))],
        compiler_params=params(), cost_estimate=cost(2 * tokens * D * AW * 1.6, tokens * 8000), name="attn_fwd",
    )(raw, x, gain, cos_t, sin_t)


def mlp_fwd_kernel(chunk, raw, h_ref, gain_ref, y_ref, g_ref, u_ref, n_ref, act_ref, wgu_out, wd_out,
                   buf, wgu, wd, sems, out_sems):
    step = pl.program_id(0)
    copies = (pltpu.make_async_copy(wgu, wgu_out, out_sems.at[0]), pltpu.make_async_copy(wd, wd_out, out_sems.at[1]))

    @pl.when(step == 0)
    def _():
        def place(d, shard):
            wgu[d * ROWS:(d + 1) * ROWS, :] = shard[:ROWS, :2 * FF]
            for i in range(10):
                for j in range(8):
                    unit = i * 8 + j
                    r, c = (unit // 20) * 16, 2 * FF + (unit % 20) * 128
                    width = min(128, D - j * 128)
                    wd[d * SHARD_FF + i * 16:d * SHARD_FF + (i + 1) * 16, j * 128:j * 128 + width] = shard[r:r + 16, c:c + width]

        unpack_shards(raw, buf, sems, place)
        for copy in copies:
            copy.start()

    h32 = h_ref[...].astype(F32)
    normed = (h32 * inv_rms_of(h32) * gain_ref[...]).astype(BF16)
    n_ref[...] = normed.T
    y_ref[...] = h_ref[...]
    out = h32
    for lo in range(0, FF, chunk):
        g = mm(normed, wgu[:, lo:lo + chunk])
        u = mm(normed, wgu[:, FF + lo:FF + lo + chunk])
        g_ref[:, lo:lo + chunk] = g
        u_ref[:, lo:lo + chunk] = u
        act = (g * (0.5 * jnp.tanh(0.5 * g) + 0.5) * u).astype(BF16)
        act_ref[lo:lo + chunk, :] = act.T
        out = out + mm(act, wd[lo:lo + chunk, :])
    y_ref[...] = out.astype(BF16)

    @pl.when(step == pl.num_programs(0) - 1)
    def _():
        for copy in copies:
            copy.wait()


def mlp_fwd(raw, h, gain, tm=256, chunk=1280):
    tokens = h.shape[0]
    row = lambda n: pl.BlockSpec((tm, n), lambda i: (i, 0))
    col = lambda n: pl.BlockSpec((n, tm), lambda i: (0, i))
    return pl.pallas_call(
        functools.partial(mlp_fwd_kernel, chunk),
        grid=(tokens // tm,),
        in_specs=[ANY, row(D), const_spec((1, D))],
        out_specs=[row(D), row(FF), row(FF), col(D), col(FF), ANY, ANY],
        out_shape=[jax.ShapeDtypeStruct((tokens, D), BF16), jax.ShapeDtypeStruct((tokens, FF), F32), jax.ShapeDtypeStruct((tokens, FF), F32),
                   jax.ShapeDtypeStruct((D, tokens), BF16), jax.ShapeDtypeStruct((FF, tokens), BF16),
                   jax.ShapeDtypeStruct((D, 2 * FF), BF16), jax.ShapeDtypeStruct((FF, D), BF16)],
        scratch_shapes=[pltpu.VMEM((2, PAD_ROWS, MW), BF16), pltpu.VMEM((D, 2 * FF), BF16), pltpu.VMEM((FF, D), BF16),
                        pltpu.SemaphoreType.DMA((2,)), pltpu.SemaphoreType.DMA((2,))],
        compiler_params=params(), cost_estimate=cost(2 * tokens * D * MW, tokens * 30000), name="mlp_fwd",
    )(raw, h, gain)


def mlp_bwd_kernel(chunk, dy_ref, h_ref, g_ref, u_ref, gain_ref, wgu, wd, dgu_ref, dmid_ref, dgain_ref):
    step = pl.program_id(0)
    dy = dy_ref[...]
    grad_normed = jnp.zeros((dy.shape[0], D), F32)
    for lo in range(0, FF, chunk):
        grad_act = mm(dy, wd[lo:lo + chunk, :], 1, 1)
        g = g_ref[:, lo:lo + chunk]
        u = u_ref[:, lo:lo + chunk]
        sig = 0.5 * jnp.tanh(0.5 * g) + 0.5
        grad_sig = grad_act * sig
        grad_up = (grad_sig * g).astype(BF16)
        grad_gate = (grad_sig * u * (1.0 + g * (1.0 - sig))).astype(BF16)
        dgu_ref[:, lo:lo + chunk] = grad_gate
        dgu_ref[:, FF + lo:FF + lo + chunk] = grad_up
        grad_normed = grad_normed + mm(grad_gate, wgu[:, lo:lo + chunk], 1, 1) + mm(grad_up, wgu[:, FF + lo:FF + lo + chunk], 1, 1)
    h32 = h_ref[...].astype(F32)
    inv_rms = inv_rms_of(h32)
    scaled = h32 * inv_rms
    part = jnp.sum(grad_normed * scaled, axis=0, keepdims=True)

    @pl.when(step == 0)
    def _():
        dgain_ref[...] = jnp.zeros_like(dgain_ref)

    dgain_ref[...] += part
    grad_scaled = grad_normed * gain_ref[...]
    dmid_ref[...] = dy.astype(F32) + inv_rms * (grad_scaled - scaled * jnp.mean(grad_scaled * scaled, axis=-1, keepdims=True))


def mlp_bwd(dy, h, g, u, gain, wgu, wd, tm=256, chunk=1280):
    tokens = h.shape[0]
    row = lambda n: pl.BlockSpec((tm, n), lambda i: (i, 0))
    return pl.pallas_call(
        functools.partial(mlp_bwd_kernel, chunk),
        grid=(tokens // tm,),
        in_specs=[row(D), row(D), row(FF), row(FF), const_spec((1, D)), const_spec((D, 2 * FF)), const_spec((FF, D))],
        out_specs=[row(2 * FF), row(D), pl.BlockSpec((1, D), lambda i: (0, 0))],
        out_shape=[jax.ShapeDtypeStruct((tokens, 2 * FF), BF16), jax.ShapeDtypeStruct((tokens, D), F32), jax.ShapeDtypeStruct((1, D), F32)],
        compiler_params=params(), cost_estimate=cost(2 * tokens * D * MW, tokens * 40000), name="mlp_bwd",
    )(dy, h, g, u, gain, wgu, wd)


def dw_gate_up_kernel(n_t, d_ref, out_ref):
    acc = mm(n_t[...], d_ref[...])
    for r in range(DEV):
        out_ref[r, :ROWS, :] = acc[r * ROWS:(r + 1) * ROWS]


def dw_down_kernel(act_t, dy_ref, _, out_ref):
    acc = mm(act_t[...], dy_ref[...])
    for d in range(acc.shape[0] // SHARD_FF):
        for i in range(20):
            for j in range(8):
                width = min(128, D - j * 128)
                out_ref[d, j * 8:(j + 1) * 8, i * 128:i * 128 + width] = acc[d * SHARD_FF + i * 8:d * SHARD_FF + (i + 1) * 8, j * 128:j * 128 + width]


def mlp_weight_grads(n_t, act_t, dgu, dy, tn=512, tm=320):
    tokens = dy.shape[0]
    pack = pl.pallas_call(
        dw_gate_up_kernel,
        grid=(2 * FF // tn,),
        in_specs=[const_spec((D, tokens)), pl.BlockSpec((tokens, tn), lambda i: (0, i))],
        out_specs=pl.BlockSpec((DEV, PAD_ROWS, tn), lambda i: (0, 0, i)),
        out_shape=jax.ShapeDtypeStruct((DEV, PAD_ROWS, MW), F32),
        compiler_params=params(), cost_estimate=cost(2 * tokens * D * 2 * FF, tokens * 12000 + D * FF * 8), name="dw_gate_up",
    )(n_t, dgu)
    return pl.pallas_call(
        dw_down_kernel,
        grid=(FF // tm,),
        in_specs=[pl.BlockSpec((tm, tokens), lambda i: (i, 0)), const_spec((tokens, D)), ANY],
        out_specs=pl.BlockSpec((tm // SHARD_FF, PAD_ROWS, FF), lambda i: (i, 0, 2)),
        out_shape=jax.ShapeDtypeStruct((DEV, PAD_ROWS, MW), F32),
        input_output_aliases={2: 0},
        compiler_params=params(), cost_estimate=cost(2 * tokens * D * FF, tokens * 7000 + D * FF * 4), name="dw_down",
    )(act_t, dy, pack)


def attn_bwd_kernel(seqs, dmid_ref, x_ref, qkv_ref, o_ref, gain_ref, dgain_mlp_ref, cos_ref, sin_ref, wqkv_t, wo,
                    dx_ref, pack_ref, do_t, dqkv_t, dwqkv_t, dwo, dgain):
    step = pl.program_id(0)

    @pl.when(step == 0)
    def _():
        dwqkv_t[...] = jnp.zeros_like(dwqkv_t)
        dwo[...] = jnp.zeros_like(dwo)
        dgain[...] = jnp.zeros_like(dgain)

    grad_mid = dmid_ref[...]
    grad_mid_bf = grad_mid.astype(BF16)
    dwo[...] += mm(o_ref[...], grad_mid_bf)
    do_t[...] = mm(wo[...], grad_mid_bf, 1, 1).astype(BF16)
    cos, sin = cos_ref[...], sin_ref[...]
    half = HD // 2

    def unrotate(grad, row, cols):
        a, b = grad[:half], grad[half:]
        c, s = cos[:, :SEQ], sin[:, :SEQ]
        dqkv_t[row:row + half, cols] = (a * c + b * s).astype(BF16)
        dqkv_t[row + half:row + HD, cols] = (b * c - a * s).astype(BF16)

    for seq in range(seqs):
        cols = slice(seq * SEQ, (seq + 1) * SEQ)
        for kvh in range(KVH):
            k_t = qkv_ref[D + kvh * HD:D + (kvh + 1) * HD, cols]
            v_t = qkv_ref[D + KV + kvh * HD:D + KV + (kvh + 1) * HD, cols]
            q_t = group_cols(qkv_ref, kvh, seq)
            g_t = group_cols(do_t, kvh, seq)
            p_t = probs_t(k_t, q_t)
            dqkv_t[D + KV + kvh * HD:D + KV + (kvh + 1) * HD, cols] = mm(g_t, p_t, 1, 1).astype(BF16)
            dp_t = mm(v_t.T, g_t)
            p32 = p_t.astype(F32)
            ds_t = (p32 * (dp_t - jnp.sum(p32 * dp_t, axis=0, keepdims=True)) * HD ** -0.5).astype(BF16)
            dq_t = mm(k_t, ds_t)
            for g in range(GROUP):
                unrotate(dq_t[:, g * SEQ:(g + 1) * SEQ], (kvh * GROUP + g) * HD, cols)
            unrotate(mm(q_t, ds_t, 1, 1), D + kvh * HD, cols)

    x32 = x_ref[...].astype(F32)
    inv_rms = inv_rms_of(x32)
    scaled = x32 * inv_rms
    normed = (scaled * gain_ref[...]).astype(BF16)
    dwqkv_t[...] += mm(dqkv_t[...], normed)
    grad_normed = mm(dqkv_t[...].T, wqkv_t[...])
    dgain[...] += jnp.sum(grad_normed * scaled, axis=0, keepdims=True)
    grad_scaled = grad_normed * gain_ref[...]
    dx_ref[...] = (grad_mid + inv_rms * (grad_scaled - scaled * jnp.mean(grad_scaled * scaled, axis=-1, keepdims=True))).astype(BF16)

    @pl.when(step == pl.num_programs(0) - 1)
    def _():
        for lo in range(0, QKV, KV):
            part = dwqkv_t[lo:lo + KV, :].T
            for r in range(DEV):
                pack_ref[r, :ROWS, lo:lo + KV] = part[r * ROWS:(r + 1) * ROWS]
        for r in range(DEV):
            pack_ref[r, :ROWS, QKV:AW] = dwo[r * ROWS:(r + 1) * ROWS, :]
            pack_ref[r, ROWS:ROWS + 1, :ROWS] = dgain[:, r * ROWS:(r + 1) * ROWS]
            pack_ref[r, ROWS + 1:ROWS + 2, :ROWS] = dgain_mlp_ref[:, r * ROWS:(r + 1) * ROWS]


def attn_bwd(dmid, x, qkv_t, o_t, gain, dgain_mlp, cos_t, sin_t, wqkv_t, wo, seqs=2):
    tokens = x.shape[0]
    tm = seqs * SEQ
    row = pl.BlockSpec((tm, D), lambda i: (i, 0))
    col = lambda n: pl.BlockSpec((n, tm), lambda i: (0, i))
    return pl.pallas_call(
        functools.partial(attn_bwd_kernel, seqs),
        grid=(tokens // tm,),
        in_specs=[row, row, col(QKV), col(D), const_spec((1, D)), const_spec((1, D)), const_spec((HD // 2, tm)), const_spec((HD // 2, tm)),
                  const_spec((QKV, D)), const_spec((D, D))],
        out_specs=[row, pl.BlockSpec((DEV, PAD_ROWS, GAW), lambda i: (0, 0, 0))],
        out_shape=[jax.ShapeDtypeStruct((tokens, D), BF16), jax.ShapeDtypeStruct((DEV, PAD_ROWS, GAW), F32)],
        scratch_shapes=[pltpu.VMEM((D, tm), BF16), pltpu.VMEM((QKV, tm), BF16), pltpu.VMEM((QKV, D), F32), pltpu.VMEM((D, D), F32),
                        pltpu.VMEM((1, D), F32)],
        compiler_params=params(), cost_estimate=cost(2 * tokens * D * AW * 3.2, tokens * 16000), name="attn_bwd",
    )(dmid, x, qkv_t, o_t, gain, dgain_mlp, cos_t, sin_t, wqkv_t, wo)


def solution(mesh):
    shard_spec = P(None, "fsdp")
    batch_spec = P("fsdp")

    def gather(pack):
        return lax.all_gather(pack, "fsdp", axis=0, tiled=True).reshape(DEV, PAD_ROWS, pack.shape[-1])

    def scatter(pack):
        return lax.psum_scatter(pack.reshape(DEV * PAD_ROWS, pack.shape[-1]), "fsdp", scatter_dimension=0, tiled=True)

    def step_body(w_query, w_key, w_value, w_out, w_gate, w_up, w_down, gain_attn, gain_mlp, rope_cos, rope_sin, x_in, y_cot):
        layers = w_query.shape[0]
        shape = x_in.shape
        cos_t = jnp.tile(rope_cos.T, (1, 2))
        sin_t = jnp.tile(rope_sin.T, (1, 2))
        packs = []
        for n in range(layers):
            gains = jnp.stack([jnp.pad(gain_attn[n], (0, AW - ROWS)), jnp.pad(gain_mlp[n], (0, AW - ROWS))])
            attn_rows = jnp.concatenate([w_query[n], w_key[n], w_value[n], w_out[n]], axis=-1)
            attn_pack = jnp.concatenate([attn_rows, gains, jnp.zeros((PAD_ROWS - ROWS - 2, AW), F32)], axis=0).astype(BF16)
            gate_up = jnp.pad(jnp.concatenate([w_gate[n], w_up[n]], axis=-1), ((0, PAD_ROWS - ROWS), (0, 0)))
            down = jnp.pad(w_down[n], ((0, 0), (0, 1024 - D))).reshape(10, 16, 8, 128).transpose(0, 2, 1, 3).reshape(4, 20, 16, 128)
            down = down.transpose(0, 2, 1, 3).reshape(PAD_ROWS, FF)
            mlp_pack = jnp.concatenate([gate_up, down], axis=-1).astype(BF16)
            packs.append((attn_pack, mlp_pack))
        hidden = x_in.reshape(-1, D)
        saved = []
        raw_attn, mlp_pack = lax.optimization_barrier((gather(packs[0][0]), packs[0][1]))
        raw_mlp = gather(mlp_pack)
        for n in range(layers):
            raw_attn, hidden = lax.optimization_barrier((raw_attn, hidden))
            gains = raw_attn[:, ROWS:ROWS + 2, :ROWS].astype(F32).transpose(1, 0, 2).reshape(2, 1, D)
            mid, qkv_t, o_t, wqkv_t, wo = attn_fwd(raw_attn, hidden, gains[0], cos_t, sin_t)
            next_mlp = None
            if n + 1 < layers:
                mid, next_packs = lax.optimization_barrier((mid, packs[n + 1]))
                raw_attn, next_mlp = gather(next_packs[0]), gather(next_packs[1])
            out, g, u, n_t, act_t, wgu, wd = mlp_fwd(raw_mlp, mid, gains[1])
            saved.append((hidden, gains, qkv_t, o_t, wqkv_t, wo, mid, g, u, n_t, act_t, wgu, wd))
            hidden, raw_mlp = out, next_mlp
        grad = y_cot.reshape(-1, D)
        reduced = [None] * layers
        for n in reversed(range(layers)):
            x, gains, qkv_t, o_t, wqkv_t, wo, mid, g, u, n_t, act_t, wgu, wd = saved[n]
            dgu, dmid, dgain_mlp = mlp_bwd(grad, mid, g, u, gains[1], wgu, wd)
            mlp_grads, dmid = lax.optimization_barrier((mlp_weight_grads(n_t, act_t, dgu, grad), dmid))
            mlp_sum = scatter(mlp_grads)
            grad, attn_grads = attn_bwd(dmid, x, qkv_t, o_t, gains[0], dgain_mlp, cos_t, sin_t, wqkv_t, wo)
            attn_sum = scatter(attn_grads)
            reduced[n] = (attn_sum, mlp_sum)

        def collect(pick):
            return jnp.stack([pick(*parts) for parts in reduced])

        def down_rows(m):
            return m[:, 2 * FF:].reshape(8, 8, 20, 128).transpose(2, 1, 0, 3).reshape(SHARD_FF, 1024)[:, :D]

        return (
            hidden.reshape(shape), grad.reshape(shape),
            collect(lambda a, m: a[:ROWS, :D]),
            collect(lambda a, m: a[:ROWS, D:D + KV]),
            collect(lambda a, m: a[:ROWS, D + KV:QKV]),
            collect(lambda a, m: a[:ROWS, QKV:AW]),
            collect(lambda a, m: m[:ROWS, :FF]),
            collect(lambda a, m: m[:ROWS, FF:2 * FF]),
            collect(lambda a, m: down_rows(m)),
            collect(lambda a, m: a[ROWS, :ROWS]),
            collect(lambda a, m: a[ROWS + 1, :ROWS]),
        )

    in_specs = (shard_spec,) * 9 + (P(), P(), batch_spec, batch_spec)
    out_specs = (batch_spec, batch_spec) + (shard_spec,) * 9
    return jax.shard_map(step_body, mesh=mesh, in_specs=in_specs, out_specs=out_specs, check_vma=False)
```

```python
import functools

import jax
import jax.numpy as jnp
from jax import lax
from jax.experimental import pallas as pl
from jax.experimental.pallas import tpu as pltpu
from jax.sharding import PartitionSpec as P


NORM_EPS = 1e-5
MASK_VALUE = -1e30
F32 = jnp.float32
BF16 = jnp.bfloat16

DEV = 16
D = 960
ROWS = D // DEV
PAD_ROWS = 64
FF = 2560
SHARD_FF = FF // DEV
KV = 320
HD = 64
KVH = 5
GROUP = 3
SEQ = 256
QKV = D + 2 * KV
AW = QKV + D
GW = 5376
GW1 = 2688
MW = 3 * FF
VMEM_LIMIT = 62 * 1024 * 1024
EXP_SCALE = HD ** -0.5 * 1.4426950408889634


def mm(a, b, ca=1, cb=0):
    return lax.dot_general(a, b, (((ca,), (cb,)), ((), ())), preferred_element_type=F32)


def params(**kw):
    return pltpu.CompilerParams(vmem_limit_bytes=VMEM_LIMIT, dimension_semantics=("arbitrary",), **kw)


def cost(flops, nbytes):
    return pl.CostEstimate(flops=int(flops), bytes_accessed=int(nbytes), transcendentals=0)


def const_spec(shape):
    zeros = (0,) * len(shape)
    return pl.BlockSpec(shape, lambda i: zeros, pipeline_mode=pl.Buffered(1))


ANY = pl.BlockSpec(memory_space=pl.ANY)


def load_tokens(ref):
    if len(ref.shape) == 2:
        return ref[...]
    return jnp.concatenate([ref[i].T for i in range(ref.shape[0])], axis=0)


def store_tokens(ref, vals):
    if len(ref.shape) == 2:
        ref[...] = vals
    else:
        for i in range(ref.shape[0]):
            ref[i] = vals[i * SEQ:(i + 1) * SEQ].T


def token_spec(tm, transposed):
    if transposed:
        return pl.BlockSpec((tm // SEQ, D, SEQ), lambda i: (i, 0, 0))
    return pl.BlockSpec((tm, D), lambda i: (i, 0))


def token_shape(tokens, transposed):
    return jax.ShapeDtypeStruct((tokens // SEQ, D, SEQ) if transposed else (tokens, D), BF16)


def inv_rms_of(vals32):
    return lax.rsqrt(jnp.mean(vals32 * vals32, axis=-1, keepdims=True) + NORM_EPS)


def unpack_shards(raw, buf, sems, place):
    def fetch(d):
        return pltpu.make_async_copy(raw.at[d], buf.at[d % 2], sems.at[d % 2])

    fetch(0).start()
    for d in range(DEV):
        if d + 1 < DEV:
            fetch(d + 1).start()
        fetch(d).wait()
        place(d, buf.at[d % 2])


HALF_SEQ = SEQ // 2


def group_cols(ref, kv_head, seq, part):
    base, lo = kv_head * GROUP * HD, seq * SEQ + part * HALF_SEQ
    return jnp.concatenate([ref[base + g * HD: base + (g + 1) * HD, lo:lo + HALF_SEQ] for g in range(GROUP)], axis=1)


def causal(scores):
    key = lax.broadcasted_iota(jnp.int32, scores.shape, 0)
    qry = lax.broadcasted_iota(jnp.int32, scores.shape, 1) & (HALF_SEQ - 1)
    return jnp.where(key <= qry, scores, MASK_VALUE)


def score_pair(keys, q_a, q_b):
    return mm(keys[:HALF_SEQ], q_a), mm(keys, q_b)


def prob_pair(scores):
    s_a = causal(scores[0] * EXP_SCALE)
    e_a = jnp.exp2(s_a - jnp.max(s_a, axis=0, keepdims=True))
    p_a = (e_a * (1.0 / jnp.sum(e_a, axis=0, keepdims=True))).astype(BF16)
    s_b = jnp.concatenate([scores[1][:HALF_SEQ] * EXP_SCALE, causal(scores[1][HALF_SEQ:] * EXP_SCALE)], axis=0)
    e_b = jnp.exp2(s_b - jnp.max(s_b, axis=0, keepdims=True))
    p_b = (e_b * (1.0 / jnp.sum(e_b, axis=0, keepdims=True))).astype(BF16)
    return p_a, p_b


def attn_fwd_kernel(seqs, raw, x_ref, gain_ref, cos_ref, sin_ref, h_ref, qkv_ref, o_ref, wqkv_out, wo_out,
                    buf, wqkv_t, wo, sems, out_sems):
    step = pl.program_id(0)
    copies = (pltpu.make_async_copy(wqkv_t, wqkv_out, out_sems.at[0]), pltpu.make_async_copy(wo, wo_out, out_sems.at[1]))

    @pl.when(step == 0)
    def _():
        def place(d, shard):
            wo[d * ROWS:(d + 1) * ROWS, :] = shard[:ROWS, QKV:]
            rows = shard[:, :QKV].T
            wqkv_t[:, d * ROWS:(d + 1) * ROWS] = rows[:, :ROWS]

        unpack_shards(raw, buf, sems, place)
        for copy in copies:
            copy.start()

    x32 = load_tokens(x_ref).astype(F32)
    normed = (x32 * inv_rms_of(x32) * gain_ref[...]).astype(BF16)
    cos, sin = cos_ref[...], sin_ref[...]
    half = HD // 2
    for lo in range(0, QKV, KV):
        part = mm(wqkv_t[lo:lo + KV, :], normed, 1, 1)
        if lo < D + KV:
            for head in range(KV // HD):
                a = part[head * HD:head * HD + half]
                b = part[head * HD + half:(head + 1) * HD]
                qkv_ref[lo + head * HD:lo + head * HD + half, :] = (a * cos - b * sin).astype(BF16)
                qkv_ref[lo + head * HD + half:lo + (head + 1) * HD, :] = (b * cos + a * sin).astype(BF16)
        else:
            qkv_ref[lo:lo + KV, :] = part.astype(BF16)
    items = [(seq, kvh) for seq in range(seqs) for kvh in range(KVH)]

    def scores_of(seq, kvh):
        keys = qkv_ref[D + kvh * HD:D + (kvh + 1) * HD, seq * SEQ:(seq + 1) * SEQ].T
        return score_pair(keys, group_cols(qkv_ref, kvh, seq, 0), group_cols(qkv_ref, kvh, seq, 1))

    scores = scores_of(*items[0])
    for pos, (seq, kvh) in enumerate(items):
        ahead = scores_of(*items[pos + 1]) if pos + 1 < len(items) else None
        probs = prob_pair(scores)
        scores = ahead
        v_t = qkv_ref[D + KV + kvh * HD:D + KV + (kvh + 1) * HD, seq * SEQ:(seq + 1) * SEQ]
        for part in range(2):
            o_t = mm(v_t[:, :(part + 1) * HALF_SEQ], probs[part]).astype(BF16)
            lo = seq * SEQ + part * HALF_SEQ
            for g in range(GROUP):
                row = (kvh * GROUP + g) * HD
                o_ref[row:row + HD, lo:lo + HALF_SEQ] = o_t[:, g * HALF_SEQ:(g + 1) * HALF_SEQ]
    h_ref[...] = (x32 + mm(o_ref[...].T, wo[...])).astype(BF16)

    @pl.when(step == pl.num_programs(0) - 1)
    def _():
        for copy in copies:
            copy.wait()


def attn_fwd(raw, x, gain, cos_t, sin_t, seqs=2):
    tokens = x.size // D
    tm = seqs * SEQ
    row = pl.BlockSpec((tm, D), lambda i: (i, 0))
    col = lambda n: pl.BlockSpec((n, tm), lambda i: (0, i))
    return pl.pallas_call(
        functools.partial(attn_fwd_kernel, seqs),
        grid=(tokens // tm,),
        in_specs=[ANY, token_spec(tm, x.ndim == 3), const_spec((1, D)), const_spec((HD // 2, tm)), const_spec((HD // 2, tm))],
        out_specs=[row, col(QKV), col(D), ANY, ANY],
        out_shape=[jax.ShapeDtypeStruct((tokens, D), BF16), jax.ShapeDtypeStruct((QKV, tokens), BF16),
                   jax.ShapeDtypeStruct((D, tokens), BF16), jax.ShapeDtypeStruct((QKV, D), BF16), jax.ShapeDtypeStruct((D, D), BF16)],
        scratch_shapes=[pltpu.VMEM((2, PAD_ROWS, AW), BF16), pltpu.VMEM((QKV, D), BF16), pltpu.VMEM((D, D), BF16),
                        pltpu.SemaphoreType.DMA((2,)), pltpu.SemaphoreType.DMA((2,))],
        compiler_params=params(), cost_estimate=cost(2 * tokens * D * AW * 1.6, tokens * 8000), name="attn_fwd",
    )(raw, x, gain, cos_t, sin_t)


def mlp_fwd_kernel(chunk, raw, h_ref, gain_ref, y_ref, g_ref, u_ref, n_ref, act_ref, wgu_out, wd_out,
                   buf, wgu, wd, sems, out_sems):
    step = pl.program_id(0)
    copies = (pltpu.make_async_copy(wgu, wgu_out, out_sems.at[0]), pltpu.make_async_copy(wd, wd_out, out_sems.at[1]))

    @pl.when(step == 0)
    def _():
        def place(d, shard):
            wgu[d * ROWS:(d + 1) * ROWS, :] = shard[:ROWS, :2 * FF]
            for i in range(10):
                for j in range(8):
                    unit = i * 8 + j
                    r, c = (unit // 20) * 16, 2 * FF + (unit % 20) * 128
                    width = min(128, D - j * 128)
                    wd[d * SHARD_FF + i * 16:d * SHARD_FF + (i + 1) * 16, j * 128:j * 128 + width] = shard[r:r + 16, c:c + width]

        unpack_shards(raw, buf, sems, place)
        for copy in copies:
            copy.start()

    h32 = h_ref[...].astype(F32)
    normed = (h32 * inv_rms_of(h32) * gain_ref[...]).astype(BF16)
    n_ref[...] = normed.T
    out = h32
    for lo in range(0, FF, chunk):
        g = mm(normed, wgu[:, lo:lo + chunk])
        u = mm(normed, wgu[:, FF + lo:FF + lo + chunk])
        g_ref[:, lo:lo + chunk] = g
        u_ref[:, lo:lo + chunk] = u
        act = (g * (0.5 * jnp.tanh(0.5 * g) + 0.5) * u).astype(BF16)
        act_ref[lo:lo + chunk, :] = act.T
        out = out + mm(act, wd[lo:lo + chunk, :])
    store_tokens(y_ref, out.astype(BF16))

    @pl.when(step == pl.num_programs(0) - 1)
    def _():
        for copy in copies:
            copy.wait()


def mlp_fwd(raw, h, gain, transposed, tm=256, chunk=1280):
    tokens = h.shape[0]
    row = lambda n: pl.BlockSpec((tm, n), lambda i: (i, 0))
    col = lambda n: pl.BlockSpec((n, tm), lambda i: (0, i))
    return pl.pallas_call(
        functools.partial(mlp_fwd_kernel, chunk),
        grid=(tokens // tm,),
        in_specs=[ANY, row(D), const_spec((1, D))],
        out_specs=[token_spec(tm, transposed), row(FF), row(FF), col(D), col(FF), ANY, ANY],
        out_shape=[token_shape(tokens, transposed), jax.ShapeDtypeStruct((tokens, FF), F32), jax.ShapeDtypeStruct((tokens, FF), F32),
                   jax.ShapeDtypeStruct((D, tokens), BF16), jax.ShapeDtypeStruct((FF, tokens), BF16),
                   jax.ShapeDtypeStruct((D, 2 * FF), BF16), jax.ShapeDtypeStruct((FF, D), BF16)],
        scratch_shapes=[pltpu.VMEM((2, PAD_ROWS, MW), BF16), pltpu.VMEM((D, 2 * FF), BF16), pltpu.VMEM((FF, D), BF16),
                        pltpu.SemaphoreType.DMA((2,)), pltpu.SemaphoreType.DMA((2,))],
        compiler_params=params(), cost_estimate=cost(2 * tokens * D * MW, tokens * 30000), name="mlp_fwd",
    )(raw, h, gain)


def mlp_bwd_kernel(chunk, dy_ref, h_ref, g_ref, u_ref, gain_ref, wgu, wd, dgu_ref, dmid_ref, dgain_ref):
    step = pl.program_id(0)
    dy = load_tokens(dy_ref)
    grad_normed = jnp.zeros((dy.shape[0], D), F32)
    for lo in range(0, FF, chunk):
        grad_act = mm(dy, wd[lo:lo + chunk, :], 1, 1)
        g = g_ref[:, lo:lo + chunk]
        u = u_ref[:, lo:lo + chunk]
        sig = 0.5 * jnp.tanh(0.5 * g) + 0.5
        grad_sig = grad_act * sig
        grad_up = (grad_sig * g).astype(BF16)
        grad_gate = (grad_sig * u * (1.0 + g * (1.0 - sig))).astype(BF16)
        dgu_ref[:, lo:lo + chunk] = grad_gate
        dgu_ref[:, FF + lo:FF + lo + chunk] = grad_up
        grad_normed = grad_normed + mm(grad_gate, wgu[:, lo:lo + chunk], 1, 1) + mm(grad_up, wgu[:, FF + lo:FF + lo + chunk], 1, 1)
    h32 = h_ref[...].astype(F32)
    inv_rms = inv_rms_of(h32)
    scaled = h32 * inv_rms
    part = jnp.sum(grad_normed * scaled, axis=0, keepdims=True)

    @pl.when(step == 0)
    def _():
        dgain_ref[...] = jnp.zeros_like(dgain_ref)

    dgain_ref[...] += part
    grad_scaled = grad_normed * gain_ref[...]
    dmid_ref[...] = dy.astype(F32) + inv_rms * (grad_scaled - scaled * jnp.mean(grad_scaled * scaled, axis=-1, keepdims=True))


def mlp_bwd(dy, h, g, u, gain, wgu, wd, tm=256, chunk=1280):
    tokens = h.shape[0]
    row = lambda n: pl.BlockSpec((tm, n), lambda i: (i, 0))
    return pl.pallas_call(
        functools.partial(mlp_bwd_kernel, chunk),
        grid=(tokens // tm,),
        in_specs=[token_spec(tm, dy.ndim == 3), row(D), row(FF), row(FF), const_spec((1, D)), const_spec((D, 2 * FF)), const_spec((FF, D))],
        out_specs=[row(2 * FF), row(D), pl.BlockSpec((1, D), lambda i: (0, 0))],
        out_shape=[jax.ShapeDtypeStruct((tokens, 2 * FF), BF16), jax.ShapeDtypeStruct((tokens, D), F32), jax.ShapeDtypeStruct((1, D), F32)],
        compiler_params=params(), cost_estimate=cost(2 * tokens * D * MW, tokens * 40000), name="mlp_bwd",
    )(dy, h, g, u, gain, wgu, wd)


def dw_gate_up_kernel(n_t, d_ref, out_ref):
    acc = mm(n_t[...], d_ref[...])
    for r in range(DEV):
        out_ref[r, :ROWS, :] = acc[r * ROWS:(r + 1) * ROWS]


def dw_down_kernel(turned, act_t, dy_ref, *refs):
    if turned:
        out_ref, rows = refs[-2:]

        @pl.when(pl.program_id(0) == 0)
        def _():
            for i in range(dy_ref.shape[0]):
                rows[i * SEQ:(i + 1) * SEQ, :] = dy_ref[i].T
    else:
        out_ref, rows = refs[-1], dy_ref
    acc = mm(act_t[...], rows[...])
    for d in range(acc.shape[0] // SHARD_FF):
        for i in range(20):
            for j in range(8):
                width = min(128, D - j * 128)
                out_ref[d, j * 8:(j + 1) * 8, i * 128:i * 128 + width] = acc[d * SHARD_FF + i * 8:d * SHARD_FF + (i + 1) * 8, j * 128:j * 128 + width]


def dw_gate_up(n_t, dgu, tn=512):
    tokens = dgu.shape[0]
    return pl.pallas_call(
        dw_gate_up_kernel,
        grid=(2 * FF // tn,),
        in_specs=[const_spec((D, tokens)), pl.BlockSpec((tokens, tn), lambda i: (0, i))],
        out_specs=pl.BlockSpec((DEV, PAD_ROWS, tn), lambda i: (0, 0, i)),
        out_shape=jax.ShapeDtypeStruct((DEV, PAD_ROWS, GW), F32),
        compiler_params=params(), cost_estimate=cost(2 * tokens * D * 2 * FF, tokens * 12000 + D * FF * 8), name="dw_gate_up",
    )(n_t, dgu)


def dw_down(act_t, dy, pack=None, tm=320):
    tokens = act_t.shape[1]
    turned, joined = dy.ndim == 3, pack is not None
    return pl.pallas_call(
        functools.partial(dw_down_kernel, turned),
        grid=(FF // tm,),
        in_specs=[pl.BlockSpec((tm, tokens), lambda i: (i, 0)), const_spec(dy.shape)] + [ANY] * joined,
        out_specs=pl.BlockSpec((tm // SHARD_FF, PAD_ROWS, FF), lambda i: (i, 0, 1 if joined else 0)),
        out_shape=jax.ShapeDtypeStruct((DEV, PAD_ROWS, GW if joined else GW1), F32),
        input_output_aliases={2: 0} if joined else {},
        scratch_shapes=[pltpu.VMEM((tokens, D), BF16)] * turned,
        compiler_params=params(), cost_estimate=cost(2 * tokens * D * FF, tokens * 7000 + D * FF * 4), name="dw_down",
    )(act_t, dy, *((pack,) if joined else ()))


def attn_bwd_kernel(seqs, dmid_ref, x_ref, qkv_ref, o_ref, gain_ref, dgain_mlp_ref, cos_ref, sin_ref, wqkv_t, wo,
                    dx_ref, pack_ref, do_t, dqkv_t, dwqkv_t, dwo, dgain):
    step = pl.program_id(0)

    @pl.when(step == 0)
    def _():
        dwqkv_t[...] = jnp.zeros_like(dwqkv_t)
        dwo[...] = jnp.zeros_like(dwo)
        dgain[...] = jnp.zeros_like(dgain)

    grad_mid = dmid_ref[...]
    grad_mid_bf = grad_mid.astype(BF16)
    dwo[...] += mm(o_ref[...], grad_mid_bf)
    do_t[...] = mm(wo[...], grad_mid_bf, 1, 1).astype(BF16)
    cos, sin = cos_ref[...], sin_ref[...]
    half = HD // 2

    def unrotate(grad, row, lo, pos):
        n = grad.shape[1]
        a, b = grad[:half], grad[half:]
        c, s = cos[:, pos:pos + n], sin[:, pos:pos + n]
        dqkv_t[row:row + half, lo:lo + n] = (a * c + b * s).astype(BF16)
        dqkv_t[row + half:row + HD, lo:lo + n] = (b * c - a * s).astype(BF16)

    items = [(seq, kvh) for seq in range(seqs) for kvh in range(KVH)]

    def loads(seq, kvh):
        cols = slice(seq * SEQ, (seq + 1) * SEQ)
        k_t = qkv_ref[D + kvh * HD:D + (kvh + 1) * HD, cols]
        v_t = qkv_ref[D + KV + kvh * HD:D + KV + (kvh + 1) * HD, cols]
        q = [group_cols(qkv_ref, kvh, seq, part) for part in range(2)]
        g = [group_cols(do_t, kvh, seq, part) for part in range(2)]
        return k_t, q, g, score_pair(k_t.T, *q), score_pair(v_t.T, *g)

    def grad_scores(p, dp):
        p32 = p.astype(F32)
        return (p32 * (dp - jnp.sum(p32 * dp, axis=0, keepdims=True)) * HD ** -0.5).astype(BF16)

    def both(lhs, rhs):
        early, full = mm(lhs[0], rhs[0], 1, 1), mm(lhs[1], rhs[1], 1, 1)
        return jnp.concatenate([early + full[:, :HALF_SEQ], full[:, HALF_SEQ:]], axis=1)

    now = loads(*items[0])
    for pos, (seq, kvh) in enumerate(items):
        ahead = loads(*items[pos + 1]) if pos + 1 < len(items) else None
        k_t, q, g, scores, dp = now
        now = ahead
        p = prob_pair(scores)
        ds = [grad_scores(p[part], dp[part]) for part in range(2)]
        lo = seq * SEQ
        dqkv_t[D + KV + kvh * HD:D + KV + (kvh + 1) * HD, lo:lo + SEQ] = both(g, p).astype(BF16)
        for part in range(2):
            dq_t = mm(k_t[:, :(part + 1) * HALF_SEQ], ds[part])
            for head in range(GROUP):
                unrotate(dq_t[:, head * HALF_SEQ:(head + 1) * HALF_SEQ], (kvh * GROUP + head) * HD, lo + part * HALF_SEQ, part * HALF_SEQ)
        unrotate(both(q, ds), D + kvh * HD, lo, 0)

    x32 = load_tokens(x_ref).astype(F32)
    inv_rms = inv_rms_of(x32)
    scaled = x32 * inv_rms
    normed = (scaled * gain_ref[...]).astype(BF16)
    dwqkv_t[...] += mm(dqkv_t[...], normed)
    grad_normed = mm(dqkv_t[...].T, wqkv_t[...])
    dgain[...] += jnp.sum(grad_normed * scaled, axis=0, keepdims=True)
    grad_scaled = grad_normed * gain_ref[...]
    store_tokens(dx_ref, (grad_mid + inv_rms * (grad_scaled - scaled * jnp.mean(grad_scaled * scaled, axis=-1, keepdims=True))).astype(BF16))

    @pl.when(step == pl.num_programs(0) - 1)
    def _():
        for lo in range(0, QKV, KV):
            part = dwqkv_t[lo:lo + KV, :].T
            for r in range(DEV):
                pack_ref[r, :ROWS, lo:lo + KV] = part[r * ROWS:(r + 1) * ROWS]
        for r in range(DEV):
            pack_ref[r, :ROWS, QKV:AW] = dwo[r * ROWS:(r + 1) * ROWS, :]
            pack_ref[r, ROWS:ROWS + 1, :ROWS] = dgain[:, r * ROWS:(r + 1) * ROWS]
            pack_ref[r, ROWS + 1:ROWS + 2, :ROWS] = dgain_mlp_ref[:, r * ROWS:(r + 1) * ROWS]


def attn_bwd(dmid, x, qkv_t, o_t, gain, dgain_mlp, cos_t, sin_t, wqkv_t, wo, width, seqs=2):
    tokens = dmid.shape[0]
    tm = seqs * SEQ
    row = pl.BlockSpec((tm, D), lambda i: (i, 0))
    col = lambda n: pl.BlockSpec((n, tm), lambda i: (0, i))
    return pl.pallas_call(
        functools.partial(attn_bwd_kernel, seqs),
        grid=(tokens // tm,),
        in_specs=[row, token_spec(tm, x.ndim == 3), col(QKV), col(D), const_spec((1, D)), const_spec((1, D)), const_spec((HD // 2, tm)),
                  const_spec((HD // 2, tm)), const_spec((QKV, D)), const_spec((D, D))],
        out_specs=[token_spec(tm, x.ndim == 3), pl.BlockSpec((DEV, PAD_ROWS, AW), lambda i: (0, 0, 0))],
        out_shape=[token_shape(tokens, x.ndim == 3), jax.ShapeDtypeStruct((DEV, PAD_ROWS, width), F32)],
        scratch_shapes=[pltpu.VMEM((D, tm), BF16), pltpu.VMEM((QKV, tm), BF16), pltpu.VMEM((QKV, D), F32), pltpu.VMEM((D, D), F32),
                        pltpu.VMEM((1, D), F32)],
        compiler_params=params(), cost_estimate=cost(2 * tokens * D * AW * 3.2, tokens * 16000), name="attn_bwd",
    )(dmid, x, qkv_t, o_t, gain, dgain_mlp, cos_t, sin_t, wqkv_t, wo)


def solution(mesh):
    shard_spec = P(None, "fsdp")
    batch_spec = P("fsdp")

    def gather(pack):
        return lax.all_gather(pack, "fsdp", axis=0, tiled=True).reshape(DEV, PAD_ROWS, pack.shape[-1])

    def scatter(pack):
        return lax.psum_scatter(pack.reshape(DEV * PAD_ROWS, pack.shape[-1]), "fsdp", scatter_dimension=0, tiled=True)

    def step_body(w_query, w_key, w_value, w_out, w_gate, w_up, w_down, gain_attn, gain_mlp, rope_cos, rope_sin, x_in, y_cot):
        layers = w_query.shape[0]
        cos_t = jnp.tile(rope_cos.T, (1, 2))
        sin_t = jnp.tile(rope_sin.T, (1, 2))
        packs = []
        for n in range(layers):
            gains = jnp.stack([jnp.pad(gain_attn[n], (0, AW - ROWS)), jnp.pad(gain_mlp[n], (0, AW - ROWS))])
            attn_rows = jnp.concatenate([w_query[n], w_key[n], w_value[n], w_out[n]], axis=-1)
            attn_pack = jnp.concatenate([attn_rows, gains, jnp.zeros((PAD_ROWS - ROWS - 2, AW), F32)], axis=0).astype(BF16)
            gate_up = jnp.pad(jnp.concatenate([w_gate[n], w_up[n]], axis=-1), ((0, PAD_ROWS - ROWS), (0, 0)))
            down = jnp.pad(w_down[n], ((0, 0), (0, 1024 - D))).reshape(10, 16, 8, 128).transpose(0, 2, 1, 3).reshape(4, 20, 16, 128)
            down = down.transpose(0, 2, 1, 3).reshape(PAD_ROWS, FF)
            mlp_pack = jnp.concatenate([gate_up, down], axis=-1).astype(BF16)
            packs.append((attn_pack, mlp_pack))
        hidden = x_in.transpose(0, 2, 1)
        saved = []
        raw_attn, mlp_pack = lax.optimization_barrier((gather(packs[0][0]), packs[0][1]))
        raw_mlp = gather(mlp_pack)
        for n in range(layers):
            raw_attn, hidden = lax.optimization_barrier((raw_attn, hidden))
            gains = raw_attn[:, ROWS:ROWS + 2, :ROWS].astype(F32).transpose(1, 0, 2).reshape(2, 1, D)
            mid, qkv_t, o_t, wqkv_t, wo = attn_fwd(raw_attn, hidden, gains[0], cos_t, sin_t)
            next_mlp = None
            if n + 1 < layers:
                mid, next_packs = lax.optimization_barrier((mid, packs[n + 1]))
                raw_attn, next_mlp = gather(next_packs[0]), gather(next_packs[1])
            out, g, u, n_t, act_t, wgu, wd = mlp_fwd(raw_mlp, mid, gains[1], n + 1 == layers)
            saved.append((hidden, gains, qkv_t, o_t, wqkv_t, wo, mid, g, u, n_t, act_t, wgu, wd))
            hidden, raw_mlp = out, next_mlp
        grad = y_cot.transpose(0, 2, 1)
        gate_up_sums, attn_sums, down_sums = [None] * layers, [None] * layers, [None] * layers
        attn_grads = None
        for n in reversed(range(layers)):
            x, gains, qkv_t, o_t, wqkv_t, wo, mid, g, u, n_t, act_t, wgu, wd = saved[n]
            pack = dw_down(act_t, grad, attn_grads)
            pack, grad = lax.optimization_barrier((pack, grad))
            down_sum = scatter(pack)
            if attn_grads is None:
                down_sums[n] = down_sum[:, :FF]
            else:
                attn_sums[n + 1], down_sums[n] = down_sum[:, :AW], down_sum[:, AW:AW + FF]
            dgu, dmid, dgain_mlp = mlp_bwd(grad, mid, g, u, gains[1], wgu, wd)
            gate_up_grads, dmid = lax.optimization_barrier((dw_gate_up(n_t, dgu), dmid))
            gate_up_sums[n] = scatter(gate_up_grads)
            grad, attn_grads = attn_bwd(dmid, x, qkv_t, o_t, gains[0], dgain_mlp, cos_t, sin_t, wqkv_t, wo, GW if n > 0 else GW1)
        attn_sums[0] = scatter(attn_grads)

        def collect(pick):
            return jnp.stack([pick(*parts) for parts in zip(attn_sums, gate_up_sums, down_sums)])

        def down_rows(m):
            return m.reshape(8, 8, 20, 128).transpose(2, 1, 0, 3).reshape(SHARD_FF, 1024)[:, :D]

        return (
            hidden.transpose(0, 2, 1), grad.transpose(0, 2, 1),
            collect(lambda a, m, d: a[:ROWS, :D]),
            collect(lambda a, m, d: a[:ROWS, D:D + KV]),
            collect(lambda a, m, d: a[:ROWS, D + KV:QKV]),
            collect(lambda a, m, d: a[:ROWS, QKV:AW]),
            collect(lambda a, m, d: m[:ROWS, :FF]),
            collect(lambda a, m, d: m[:ROWS, FF:2 * FF]),
            collect(lambda a, m, d: down_rows(d)),
            collect(lambda a, m, d: a[ROWS, :ROWS]),
            collect(lambda a, m, d: a[ROWS + 1, :ROWS]),
        )

    in_specs = (shard_spec,) * 9 + (P(), P(), batch_spec, batch_spec)
    out_specs = (batch_spec, batch_spec) + (shard_spec,) * 9
    return jax.shard_map(step_body, mesh=mesh, in_specs=in_specs, out_specs=out_specs, check_vma=False)
```
